8 devices in a mesh: dp: 1 (over z), sp: 8 (over y, x, core).
Axes of the slice: x: 2, y: 2, z: 1, core: 2. Of those that a mesh axis runs over, the one named last changes fastest.
Arguments:
- hidden: bfloat16 [2048, 2048], P(('dp', 'sp'))
- seg_ids: int32 [2048], P(('dp', 'sp'))
- norm_kv: bfloat16 [2048], replicated
- w_key: bfloat16 [2048, 32, 64], replicated
- w_value: bfloat16 [2048, 32, 64], replicated
- norm_attn: bfloat16 [1, 2048], replicated
- w_query: bfloat16 [1, 2048, 32, 64], replicated
- w_out: bfloat16 [1, 32, 64, 2048], replicated
- norm_mlp: bfloat16 [1, 2048], replicated
- w_gate: bfloat16 [1, 2048, 8192], replicated
- w_up: bfloat16 [1, 2048, 8192], replicated
- w_down: bfloat16 [1, 8192, 2048], replicated
Outputs:
- output: bfloat16 [2048, 2048], P(('dp', 'sp'))
All inputs are finite; a program needn't handle non-finite values.
Results may differ from the reference program's by a relative error of at most 0.0132325.
Values are sent between devices in bfloat16 or wider.
A program may use at most 1 GiB of HBM per device.

```python
import math
import jax
import jax.numpy as jnp
from jax import lax

D_MODEL = 2048
Q_HEADS = 32
KV_HEADS = 32
HEAD_DIM = 64
FF_DIM = 8192
LAYERS = 1
TOKENS_DEV = 256
SHARDS = 8
SEQ_LEN = 2048
BOUNDS = 3
Q_PER_KV = Q_HEADS // KV_HEADS
NORM_EPS = 1e-6


def rms_norm(values, gain):
    val32 = values.astype(jnp.float32)
    inv_rms = lax.rsqrt(jnp.mean(val32 * val32, axis=-1, keepdims=True) + NORM_EPS)
    return (val32 * inv_rms * gain.astype(jnp.float32)).astype(jnp.bfloat16)


def draw_seg(key):
    positions = jnp.arange(SEQ_LEN, dtype=jnp.int32)
    starts = jax.random.permutation(key, SEQ_LEN - 1)[:BOUNDS].astype(jnp.int32) + 1
    return jnp.sum((positions[:, None] >= starts[None, :]).astype(jnp.int32), axis=1).astype(jnp.int32)


def setup_inputs(seed: int = 0, part: int = 0) -> dict:
    keys = jax.random.split(jax.random.key(seed), 12)
    query_gain = max(1.5, math.sqrt(math.log(SEQ_LEN / (BOUNDS + 1))))

    def draw_normal(key, shape, scale):
        return (scale * jax.random.normal(key, shape, jnp.float32)).astype(jnp.bfloat16)

    def draw_gain(key, shape):
        return (1.0 + 0.25 * jax.random.normal(key, shape, jnp.float32)).astype(jnp.bfloat16)

    hidden = draw_normal(jax.random.fold_in(keys[0], part), (SEQ_LEN, D_MODEL), 1.0)
    seg_ids = draw_seg(jax.random.fold_in(keys[1], part))
    return {
        'hidden': hidden,
        'seg_ids': seg_ids,
        'norm_kv': draw_gain(keys[2], (D_MODEL,)),
        'w_key': draw_normal(keys[3], (D_MODEL, KV_HEADS, HEAD_DIM), D_MODEL ** -0.5),
        'w_value': draw_normal(keys[4], (D_MODEL, KV_HEADS, HEAD_DIM), D_MODEL ** -0.5),
        'norm_attn': draw_gain(keys[5], (LAYERS, D_MODEL)),
        'w_query': draw_normal(keys[6], (LAYERS, D_MODEL, Q_HEADS, HEAD_DIM), query_gain * D_MODEL ** -0.5),
        'w_out': draw_normal(keys[7], (LAYERS, Q_HEADS, HEAD_DIM, D_MODEL), (Q_HEADS * HEAD_DIM) ** -0.5),
        'norm_mlp': draw_gain(keys[8], (LAYERS, D_MODEL)),
        'w_gate': draw_normal(keys[9], (LAYERS, D_MODEL, FF_DIM), D_MODEL ** -0.5),
        'w_up': draw_normal(keys[10], (LAYERS, D_MODEL, FF_DIM), D_MODEL ** -0.5),
        'w_down': draw_normal(keys[11], (LAYERS, FF_DIM, D_MODEL), FF_DIM ** -0.5),
    }


def reference(hidden, seg_ids, norm_kv, w_key, w_value, norm_attn, w_query, w_out, norm_mlp, w_gate, w_up, w_down):
    kv_width = KV_HEADS * HEAD_DIM
    q_width = Q_HEADS * HEAD_DIM
    u_kv = rms_norm(hidden, norm_kv)
    keys = jnp.dot(u_kv, w_key.reshape(D_MODEL, kv_width), preferred_element_type=jnp.float32).astype(jnp.bfloat16)
    keys = keys.reshape(SEQ_LEN, KV_HEADS, HEAD_DIM).astype(jnp.float32)
    values = jnp.dot(u_kv, w_value.reshape(D_MODEL, kv_width), preferred_element_type=jnp.float32).astype(jnp.bfloat16)
    values = values.reshape(SEQ_LEN, KV_HEADS, HEAD_DIM).astype(jnp.float32)
    positions = jnp.arange(SEQ_LEN, dtype=jnp.int32)
    blk_pos = positions.reshape(SHARDS, TOKENS_DEV)
    blk_seg = seg_ids.reshape(SHARDS, TOKENS_DEV)
    scale = HEAD_DIM ** -0.5

    def block_attention(block):
        q_blk, q_pos, q_seg = block
        scores = jnp.einsum('qrgd,kgd->grqk', q_blk, keys) * scale
        allowed = (positions[None, :] <= q_pos[:, None]) & (seg_ids[None, :] == q_seg[:, None])
        scores = jnp.where(allowed[None, None], scores, -1e30)
        probs = jax.nn.softmax(scores, axis=-1).astype(jnp.bfloat16).astype(jnp.float32)
        mixed = jnp.einsum('grqk,kgd->qrgd', probs, values)
        return mixed.astype(jnp.bfloat16).reshape(TOKENS_DEV, q_width)

    def layer_step(state, params):
        g_attn, query_w, out_w, g_mlp, gate_w, up_w, down_w = params
        u_attn = rms_norm(state, g_attn)
        query = jnp.dot(u_attn, query_w.reshape(D_MODEL, q_width), preferred_element_type=jnp.float32).astype(jnp.bfloat16)
        query = query.reshape(SHARDS, TOKENS_DEV, Q_PER_KV, KV_HEADS, HEAD_DIM).astype(jnp.float32)
        attended = lax.map(block_attention, (query, blk_pos, blk_seg)).reshape(SEQ_LEN, q_width)
        attn_out = jnp.dot(attended, out_w.reshape(q_width, D_MODEL), preferred_element_type=jnp.float32).astype(jnp.bfloat16)
        state = state + attn_out
        u_mlp = rms_norm(state, g_mlp)
        gate_val = jnp.dot(u_mlp, gate_w, preferred_element_type=jnp.float32).astype(jnp.bfloat16)
        up_val = jnp.dot(u_mlp, up_w, preferred_element_type=jnp.float32).astype(jnp.bfloat16)
        act_val = (jax.nn.silu(gate_val.astype(jnp.float32)) * up_val.astype(jnp.float32)).astype(jnp.bfloat16)
        down_val = jnp.dot(act_val, down_w, preferred_element_type=jnp.float32).astype(jnp.bfloat16)
        return state + down_val, None

    result, _ = lax.scan(layer_step, hidden, (norm_attn, w_query, w_out, norm_mlp, w_gate, w_up, w_down))
    return result
```

```python
import functools
import math
import jax
import jax.numpy as jnp
from jax import lax
from jax.experimental import pallas as pl
from jax.experimental.pallas import tpu as pltpu
from jax.sharding import PartitionSpec as P

NORM_EPS = 1e-6
MESH = pl.DeviceIdType.MESH
BF = jnp.bfloat16
F32 = jnp.float32
NEG = -1e30
T = 256
D = 2048
G = 8
FT = 512
RING = 6


def nt_dot(a, b):
    return lax.dot_general(a, b, (((1,), (1,)), ((), ())), preferred_element_type=F32)


def norm_rows(x_ref, gain_ref, out_ref, rows, step=16):
    gain = gain_ref[...].astype(F32)

    def body(i, _):
        sl = pl.ds(pl.multiple_of(i * step, step), step)
        x = x_ref[sl, :].astype(F32)
        inv = lax.rsqrt(jnp.mean(x * x, axis=-1, keepdims=True) + NORM_EPS)
        out_ref[sl, :] = (x * inv * gain).astype(BF)
        return 0

    lax.fori_loop(0, rows // step, body, 0, unroll=2)


def gather_kernel(hid, seg, gkv, gat, wk, wv, wq, k_out, v_out, q_out, seg_out,
                  hx, wk_v, wv_v, wq_v, u, kst, vst, qst,
                  w_sem, own_sem, xs, xr, ys, yr, fs, fr, seg_s, seg_r, seg_l,
                  kl, ks, kr, vl, vs, vr, q_sem):
    me = lax.axis_index("sp")
    core = lax.rem(me, 2)
    xx = lax.rem(lax.div(me, 2), 2)
    yy = lax.div(me, 4)
    sib = me + 1 - 2 * core
    xp = me + 2 - 4 * xx
    yp = me + 4 - 8 * yy
    dg = xp + 4 - 8 * yy

    own = pltpu.make_async_copy(hid, hx.at[0], own_sem)
    own.start()
    w_cp = [pltpu.make_async_copy(s, d, w_sem.at[i]) for i, (s, d) in enumerate(((wq, wq_v), (wk, wk_v), (wv, wv_v)))]
    for c in w_cp:
        c.start()
    seg_own = pltpu.make_async_copy(seg, seg_out.at[me], seg_l)
    seg_own.start()

    barrier = pltpu.get_barrier_semaphore()
    for d in range(1, 8):
        pl.semaphore_signal(barrier, inc=1, device_id={"sp": lax.rem(me + d, 8)}, device_id_type=MESH)
    pl.semaphore_wait(barrier, 7)

    def send(src, dst, ss, rs, dev):
        return pltpu.make_async_remote_copy(src_ref=src, dst_ref=dst, send_sem=ss, recv_sem=rs,
                                            device_id={"sp": dev}, device_id_type=MESH)

    q4 = T // 4
    xcp, ycp = [], []
    for i in range(4):
        r = pl.ds(i * q4, q4)
        xcp.append(send(hid.at[r], hx.at[1, r], xs.at[i], xr.at[i], xp))
        ycp.append(send(hid.at[r], hx.at[2, r], ys.at[i], yr.at[i], yp))
        xcp[-1].start()
        ycp[-1].start()
    segcp = []
    for d in range(1, 8):
        segcp.append(send(seg, seg_out.at[me], seg_s.at[d - 1], seg_r.at[d - 1], lax.rem(me + d, 8)))
        segcp[-1].start()

    own.wait()
    norm_rows(hx.at[0], gat, u, T)
    w_cp[0].wait()

    def q_body(g, _):
        sl = pl.ds(pl.multiple_of(g * 256, 256), 256)
        qst[g] = nt_dot(wq_v[sl, :], u[...]).astype(BF)
        return 0

    lax.fori_loop(0, G, q_body, 0)
    qcp = pltpu.make_async_copy(qst, q_out, q_sem)
    qcp.start()

    def emit(blk, slot, src, g):
        return (pltpu.make_async_copy(kst.at[slot, g], k_out.at[blk, g], kl.at[slot, g]),
                pltpu.make_async_copy(vst.at[slot, g], v_out.at[blk, g], vl.at[slot, g]),
                send(kst.at[slot, g], k_out.at[blk, g], ks.at[slot, g], kr.at[slot, g], sib),
                send(vst.at[slot, g], v_out.at[blk, g], vs.at[slot, g], vr.at[slot, g], sib))

    def make_kv(slot, blk):
        norm_rows(hx.at[slot], gkv, u, T)

        def body(g, _):
            sl = pl.ds(pl.multiple_of(g * 256, 256), 256)
            kst[slot, g] = nt_dot(u[...], wk_v[sl, :]).astype(BF)
            vst[slot, g] = nt_dot(wv_v[sl, :], u[...]).astype(BF)

            @pl.when(g > 0)
            def _():
                for c in emit(blk, slot, None, g - 1):
                    c.start()
            return 0

        lax.fori_loop(0, G, body, 0)
        for c in emit(blk, slot, None, G - 1):
            c.start()

    w_cp[1].wait()
    w_cp[2].wait()
    make_kv(0, me)

    fcp = []
    for i in range(4):
        r = pl.ds(i * q4, q4)
        if i % 2 == 0:
            xcp[i].wait_recv()
            c = send(hx.at[1, r], hx.at[3, r], fs.at[i], fr.at[i], yp)
        else:
            ycp[i].wait_recv()
            c = send(hx.at[2, r], hx.at[3, r], fs.at[i], fr.at[i], xp)
        c.start()
        fcp.append(c)
    xcp[1].wait_recv()
    xcp[3].wait_recv()
    make_kv(1, xp)
    ycp[0].wait_recv()
    ycp[2].wait_recv()
    make_kv(2, yp)
    for c in fcp:
        c.wait_recv()
    make_kv(3, dg)

    qcp.wait()
    seg_own.wait()
    for c in segcp:
        c.wait()
    for c in xcp + ycp + fcp:
        c.wait_send()

    def drain(i, _):
        slot, g = lax.div(i, G), lax.rem(i, G)
        c = emit(me, slot, None, g)
        c[0].wait()
        c[1].wait()
        c[2].wait()
        c[3].wait()
        return 0

    lax.fori_loop(0, 4 * G, drain, 0)


def layer_kernel(seg_s, qt, k4, v4, seg_v, hid, gmlp, wo, wg, wu, wd, out,
                 qv, kb, vb, bias, acc, mm, ll, ob, hb, um, wo_v, wg_v, wu_v, wd_v, cb, dacc,
                 q_sem, kv_sem, wo_sem, w_sem):
    me = lax.axis_index("sp")
    steps = wg.shape[1] // FT
    scale = (64 ** -0.5) * math.log2(math.e)

    def kv_copies(blk, slot):
        return (pltpu.make_async_copy(k4.at[blk], kb.at[slot], kv_sem.at[slot, 0]),
                pltpu.make_async_copy(v4.at[blk], vb.at[slot], kv_sem.at[slot, 1]))

    def w_copies(t, slot):
        sl = pl.ds(pl.multiple_of(t * FT, FT), FT)
        return (pltpu.make_async_copy(wg.at[:, sl], wg_v.at[slot], w_sem.at[slot, 0]),
                pltpu.make_async_copy(wu.at[:, sl], wu_v.at[slot], w_sem.at[slot, 1]),
                pltpu.make_async_copy(wd.at[sl, :], wd_v.at[slot], w_sem.at[slot, 2]))

    qcp = pltpu.make_async_copy(qt, qv, q_sem)
    qcp.start()
    for c in kv_copies(me, 0):
        c.start()
    wocp = pltpu.make_async_copy(wo, wo_v, wo_sem)
    wocp.start(priority=1)
    for t in range(RING):
        for c in w_copies(t, t):
            c.start(priority=1)

    first = seg_s[me, 0, 0]
    low = jnp.int32(0)
    for b in range(8):
        low = low + jnp.where((b < me) & (seg_s[b, 0, T - 1] < first), 1, 0).astype(jnp.int32)
    count = me - low + 1

    acc[...] = jnp.zeros_like(acc)
    mm[...] = jnp.full_like(mm, NEG)
    ll[...] = jnp.zeros_like(ll)
    seg_q = seg_v[me]
    qcp.wait()
    zero = jnp.zeros((64, T), BF)

    def block(i, _):
        slot = lax.rem(i, 2)
        blk = me - i

        @pl.when(i + 1 < count)
        def _():
            for c in kv_copies(blk - 1, 1 - slot):
                c.start()

        seg_k = jnp.broadcast_to(seg_v[blk], (T, T)).T
        key = lax.broadcasted_iota(jnp.int32, (T, T), 0) - i * T
        qry = lax.broadcasted_iota(jnp.int32, (T, T), 1)
        bias[...] = jnp.where((seg_k == seg_q) & (key <= qry), 0.0, NEG)
        for c in kv_copies(blk, slot):
            c.wait()

        def group(g, _):
            kg = kb[slot, g]
            for j in range(4):
                head = g * 4 + j
                qj = qv[g, j * 64:(j + 1) * 64, :]
                qw = jnp.concatenate([zero] * j + [qj] + [zero] * (3 - j), axis=0)
                s = jnp.dot(kg, qw, preferred_element_type=F32) + bias[...]
                m_old = mm[head]
                m_new = jnp.maximum(m_old, jnp.max(s, axis=0, keepdims=True))
                p = jnp.exp2(s * scale - m_new * scale)
                alpha = jnp.exp2((m_old - m_new) * scale)
                ll[head] = ll[head] * alpha + jnp.sum(p, axis=0, keepdims=True)
                mm[head] = m_new
                o = jnp.dot(vb[slot, g, j * 64:(j + 1) * 64, :], p.astype(BF), preferred_element_type=F32)
                acc[head] = acc[head] * alpha + o
            return 0

        lax.fori_loop(0, G, group, 0)
        return 0

    lax.fori_loop(0, count, block, 0)

    for g in range(G):
        parts = [acc[g * 4 + j] / ll[g * 4 + j] for j in range(4)]
        ot = jnp.concatenate(parts, axis=0)
        ob[:, g * 256:(g + 1) * 256] = ot.T.astype(BF)

    wocp.wait()

    def proj(n, _):
        sl = pl.ds(pl.multiple_of(n * 256, 256), 256)
        r = jnp.dot(ob[...], wo_v[:, sl], preferred_element_type=F32).astype(BF)
        hb[:, sl] = hid[:, sl] + r
        return 0

    lax.fori_loop(0, D // 256, proj, 0)
    norm_rows(hb, gmlp, um, T)
    dacc[...] = jnp.zeros_like(dacc)

    def front(t):
        slot = lax.rem(t, RING)
        cg, cu, _ = w_copies(t, slot)
        cg.wait()
        cu.wait()
        a = jnp.dot(um[...], wg_v[slot], preferred_element_type=F32).astype(BF).astype(F32)
        b = jnp.dot(um[...], wu_v[slot], preferred_element_type=F32).astype(BF).astype(F32)
        cb[lax.rem(t, 2)] = (jax.nn.silu(a) * b).astype(BF)

    def back(t):
        slot = lax.rem(t, RING)
        w_copies(t, slot)[2].wait()
        dacc[...] += jnp.dot(cb[lax.rem(t, 2)], wd_v[slot], preferred_element_type=F32)

    front(0)

    def mlp(t, _):
        front(t)
        back(t - 1)

        @pl.when(t - 1 + RING < steps)
        def _():
            for c in w_copies(t - 1 + RING, lax.rem(t - 1, RING)):
                c.start(priority=1)
        return 0

    lax.fori_loop(1, steps, mlp, 0)
    back(steps - 1)
    out[...] = hb[...] + dacc[...].astype(BF)


def solution(mesh):
    ANY = pl.BlockSpec(memory_space=pl.ANY)
    VM = pl.BlockSpec(memory_space=pltpu.VMEM)
    SM = pl.BlockSpec(memory_space=pltpu.SMEM)
    DMA = pltpu.SemaphoreType.DMA

    def body(hidden, seg_ids, norm_kv, w_key, w_value, norm_attn, w_query, w_out, norm_mlp, w_gate, w_up, w_down):
        wk = w_key.transpose(1, 2, 0).reshape(D, D)
        wv = w_value.transpose(1, 2, 0).reshape(D, D)
        wq = w_query[0].transpose(1, 2, 0).reshape(D, D)
        seg = seg_ids.reshape(1, T)
        tile = jax.ShapeDtypeStruct((8, G, 256, 256), BF)
        k4, v4, qt, seg_all = pl.pallas_call(
            gather_kernel,
            out_shape=(tile, tile, jax.ShapeDtypeStruct((G, 256, 256), BF), jax.ShapeDtypeStruct((8, 1, T), jnp.int32)),
            in_specs=[ANY, ANY, VM, VM, ANY, ANY, ANY],
            out_specs=(ANY, ANY, ANY, ANY),
            scratch_shapes=[
                pltpu.VMEM((4, T, D), BF), pltpu.VMEM((D, D), BF), pltpu.VMEM((D, D), BF), pltpu.VMEM((D, D), BF),
                pltpu.VMEM((T, D), BF), pltpu.VMEM((4, G, 256, 256), BF), pltpu.VMEM((4, G, 256, 256), BF),
                pltpu.VMEM((G, 256, 256), BF),
                DMA((3,)), DMA, DMA((4,)), DMA((4,)), DMA((4,)), DMA((4,)), DMA((4,)), DMA((4,)),
                DMA((7,)), DMA((7,)), DMA,
                DMA((4, G)), DMA((4, G)), DMA((4, G)), DMA((4, G)), DMA((4, G)), DMA((4, G)), DMA,
            ],
            compiler_params=pltpu.CompilerParams(collective_id=0, has_side_effects=True, vmem_limit_bytes=58 * 2 ** 20),
            cost_estimate=pl.CostEstimate(flops=20 * 10 ** 9, bytes_accessed=50 * 10 ** 6, transcendentals=0),
            name="gather_kv",
        )(hidden, seg, norm_kv.reshape(1, D), norm_attn, wk, wv, wq)

        return pl.pallas_call(
            layer_kernel,
            out_shape=jax.ShapeDtypeStruct((T, D), BF),
            in_specs=[SM, ANY, ANY, ANY, VM, VM, VM, ANY, ANY, ANY, ANY],
            out_specs=VM,
            scratch_shapes=[
                pltpu.VMEM((G, 256, 256), BF), pltpu.VMEM((2, G, 256, 256), BF), pltpu.VMEM((2, G, 256, 256), BF),
                pltpu.VMEM((T, T), F32), pltpu.VMEM((32, 64, T), F32), pltpu.VMEM((32, 1, T), F32), pltpu.VMEM((32, 1, T), F32),
                pltpu.VMEM((T, D), BF), pltpu.VMEM((T, D), BF), pltpu.VMEM((T, D), BF),
                pltpu.VMEM((D, D), BF), pltpu.VMEM((RING, D, FT), BF), pltpu.VMEM((RING, D, FT), BF), pltpu.VMEM((RING, FT, D), BF),
                pltpu.VMEM((2, T, FT), BF), pltpu.VMEM((T, D), F32),
                DMA, DMA((2, 2)), DMA, DMA((RING, 3)),
            ],
            compiler_params=pltpu.CompilerParams(vmem_limit_bytes=63 * 2 ** 20),
            cost_estimate=pl.CostEstimate(flops=40 * 10 ** 9, bytes_accessed=130 * 10 ** 6, transcendentals=10 ** 7),
            name="layer",
        )(seg_all, qt, k4, v4, seg_all, hidden, norm_mlp, w_out[0].reshape(D, D), w_gate[0], w_up[0], w_down[0])

    row_spec = P(('dp', 'sp'), None)
    in_specs = (row_spec, P(('dp', 'sp'))) + (P(),) * 10
    return jax.shard_map(body, mesh=mesh, in_specs=in_specs, out_specs=row_spec, check_vma=False)
```

```python
import functools
import math
import jax
import jax.numpy as jnp
from jax import lax
from jax.experimental import pallas as pl
from jax.experimental.pallas import tpu as pltpu
from jax.sharding import PartitionSpec as P

NORM_EPS = 1e-6
MESH = pl.DeviceIdType.MESH
BF = jnp.bfloat16
F32 = jnp.float32
NEG = -1e30
T = 256
D = 2048
G = 8
FT = 512
KVS = 3
RING = 6


def nt_dot(a, b):
    return lax.dot_general(a, b, (((1,), (1,)), ((), ())), preferred_element_type=F32)


def norm_rows(x_ref, gain_ref, out_ref, rows, start=0, step=16):
    gain = gain_ref[...].astype(F32)

    def body(i, _):
        sl = pl.ds(pl.multiple_of(start + i * step, step), step)
        x = x_ref[sl, :].astype(F32)
        inv = lax.rsqrt(jnp.mean(x * x, axis=-1, keepdims=True) + NORM_EPS)
        out_ref[sl, :] = (x * inv * gain).astype(BF)
        return 0

    lax.fori_loop(0, rows // step, body, 0, unroll=2)


def gather_kernel(hid, seg, gkv, gat, wk, wv, wq, k_out, v_out, q_out, seg_out,
                  hx, wk_v, wv_v, wq_v, u, kst, vst, qst,
                  w_sem, own_sem, xs, xr, ys, yr, fs, fr, seg_s, seg_r, seg_l,
                  kl, ks, kr, vl, vs, vr, q_sem):
    me = lax.axis_index("sp")
    core = lax.rem(me, 2)
    xx = lax.rem(lax.div(me, 2), 2)
    yy = lax.div(me, 4)
    sib = me + 1 - 2 * core
    xp = me + 2 - 4 * xx
    yp = me + 4 - 8 * yy
    dg = xp + 4 - 8 * yy

    barrier = pltpu.get_barrier_semaphore()
    for d in range(1, 8):
        pl.semaphore_signal(barrier, inc=1, device_id={"sp": lax.rem(me + d, 8)}, device_id_type=MESH)
    own = pltpu.make_async_copy(hid, hx.at[0], own_sem)
    own.start()
    w_cp = [pltpu.make_async_copy(s, d, w_sem.at[i]) for i, (s, d) in enumerate(((wq, wq_v), (wk, wk_v), (wv, wv_v)))]
    for c in w_cp:
        c.start()
    seg_own = pltpu.make_async_copy(seg, seg_out.at[me], seg_l)
    seg_own.start()
    pl.semaphore_wait(barrier, 7)

    def send(src, dst, ss, rs, dev):
        return pltpu.make_async_remote_copy(src_ref=src, dst_ref=dst, send_sem=ss, recv_sem=rs,
                                            device_id={"sp": dev}, device_id_type=MESH)

    q4, half = T // 4, T // 2
    xcp, ycp = [], []
    for i in range(4):
        r = pl.ds(i * q4, q4)
        xcp.append(send(hid.at[r], hx.at[1 + i // 2, pl.ds((i % 2) * q4, q4)], xs.at[i], xr.at[i], xp))
        ycp.append(send(hid.at[r], hx.at[1 + i // 2, pl.ds(half + (i % 2) * q4, q4)], ys.at[i], yr.at[i], yp))
        xcp[-1].start()
        ycp[-1].start()
    segcp = []
    for d in range(1, 8):
        segcp.append(send(seg, seg_out.at[me], seg_s.at[d - 1], seg_r.at[d - 1], lax.rem(me + d, 8)))
        segcp[-1].start()

    own.wait()
    norm_rows(hx.at[0], gat, u, T)
    w_cp[0].wait()

    def q_body(g, _):
        for k in range(2):
            sl = pl.ds(pl.multiple_of(g * 512 + k * 256, 256), 256)
            qst[2 * g + k] = nt_dot(wq_v[sl, :], u[...]).astype(BF)
        return 0

    lax.fori_loop(0, G // 2, q_body, 0)
    qcp = pltpu.make_async_copy(qst, q_out, q_sem)
    qcp.start()

    def to_sibling(slot, st, parts):
        res = []
        for h in range(2):
            gs = pl.ds(st * 2, 2)
            res.append(send(kst.at[slot, h, gs], k_out.at[parts[h], gs], ks.at[slot, st, h], kr.at[slot, st, h], sib))
            res.append(send(vst.at[slot, h, gs], v_out.at[parts[h], gs], vs.at[slot, st, h], vr.at[slot, st, h], sib))
        return res

    def to_self(slot, parts):
        res = []
        for h in range(2):
            res.append(pltpu.make_async_copy(kst.at[slot, h], k_out.at[parts[h]], kl.at[slot, h]))
            res.append(pltpu.make_async_copy(vst.at[slot, h], v_out.at[parts[h]], vl.at[slot, h]))
        return res

    def make_kv(slot, parts):
        def body(st, _):
            @pl.when(st > 0)
            def _():
                for c in to_sibling(slot, st - 1, parts):
                    c.start()

            for k in range(2):
                g = st * 2 + k
                sl = pl.ds(pl.multiple_of(g * 256, 256), 256)
                kk = nt_dot(u[...], wk_v[sl, :]).astype(BF)
                vv = nt_dot(wv_v[sl, :], u[...]).astype(BF)
                for h in range(2):
                    kst[slot, h, g] = kk[h * half:(h + 1) * half, :]
                    vst[slot, h, g] = vv[:, h * half:(h + 1) * half]
            return 0

        lax.fori_loop(0, G // 2, body, 0)
        for c in to_sibling(slot, G // 2 - 1, parts) + to_self(slot, parts):
            c.start()

    norm_rows(hx.at[0], gkv, u, T)
    w_cp[1].wait()
    w_cp[2].wait()
    make_kv(0, (2 * me, 2 * me + 1))

    def forward(i):
        if i % 2 == 0:
            xcp[i].wait_recv()
            src, dev = hx.at[1 + i // 2, pl.ds(0, q4)], yp
        else:
            ycp[i].wait_recv()
            src, dev = hx.at[1 + i // 2, pl.ds(half + q4, q4)], xp
        c = send(src, hx.at[3, pl.ds(i * q4, q4)], fs.at[i], fr.at[i], dev)
        c.start()
        return c

    fcp = [forward(0), forward(1)]
    xcp[1].wait_recv()
    ycp[0].wait_recv()
    norm_rows(hx.at[1], gkv, u, T)
    make_kv(1, (2 * xp, 2 * yp))
    fcp += [forward(2), forward(3)]
    xcp[3].wait_recv()
    ycp[2].wait_recv()
    norm_rows(hx.at[2], gkv, u, T)
    make_kv(2, (2 * xp + 1, 2 * yp + 1))
    fcp[0].wait_recv()
    fcp[1].wait_recv()
    norm_rows(hx.at[3], gkv, u, half)
    fcp[2].wait_recv()
    fcp[3].wait_recv()
    norm_rows(hx.at[3], gkv, u, half, half)
    make_kv(3, (2 * dg, 2 * dg + 1))

    qcp.wait()
    seg_own.wait()
    for c in segcp:
        c.wait()
    for c in xcp + ycp + fcp:
        c.wait_send()

    def drain(i, _):
        slot, st = lax.div(i, G // 2), lax.rem(i, G // 2)
        for c in to_sibling(slot, st, (2 * me, 2 * me + 1)):
            c.wait()
        return 0

    lax.fori_loop(0, 4 * (G // 2), drain, 0)
    for slot in range(4):
        for c in to_self(slot, (2 * me, 2 * me + 1)):
            c.wait()


def layer_kernel(seg_s, qt, k4, v4, seg_v, hid, gmlp, wo, wg, wu, wd, out,
                 qv, kb, vb, bias, acc, mm, ll, mx, ob, hb, um, wo_v, wg_v, wu_v, wd_v, cb, work,
                 q_sem, kv_sem, wo_sem, w_sem, h_sem, o_sem):
    me = lax.axis_index("sp")
    steps = wg.shape[1] // FT
    scale = (64 ** -0.5) * math.log2(math.e)

    def kv_copies(blk, slot):
        two = pl.ds(2 * blk, 2)
        return (pltpu.make_async_copy(k4.at[two], kb.at[slot], kv_sem.at[slot, 0]),
                pltpu.make_async_copy(v4.at[two], vb.at[slot], kv_sem.at[slot, 1]))

    def front_copies(t, slot):
        sl = pl.ds(pl.multiple_of(t * FT, FT), FT)
        return (pltpu.make_async_copy(wg.at[:, sl], wg_v.at[slot], w_sem.at[slot, 0]),
                pltpu.make_async_copy(wu.at[:, sl], wu_v.at[slot], w_sem.at[slot, 1]))

    def back_copy(t, slot):
        sl = pl.ds(pl.multiple_of(t * FT, FT), FT)
        return pltpu.make_async_copy(wd.at[sl, :], wd_v.at[slot], w_sem.at[slot, 2])

    def start_weights(t, slot):
        for c in front_copies(t, slot):
            c.start(priority=1)
        back_copy(t, slot).start(priority=1)

    qcp = pltpu.make_async_copy(qt, qv, q_sem)
    qcp.start()
    for c in kv_copies(me, 0):
        c.start()
    hcp = pltpu.make_async_copy(hid, hb, h_sem)
    hcp.start()

    first = seg_s[me, 0, 0]
    low = jnp.int32(0)
    for b in range(8):
        low = low + jnp.where((b < me) & (seg_s[b, 0, T - 1] < first), 1, 0).astype(jnp.int32)
    count = me - low + 1

    @pl.when(count > 1)
    def _():
        for c in kv_copies(me - 1, 1):
            c.start()

    wocp = pltpu.make_async_copy(wo, wo_v, wo_sem)
    wocp.start(priority=1)

    acc[...] = jnp.zeros_like(acc)
    mm[...] = jnp.full_like(mm, NEG)
    ll[...] = jnp.zeros_like(ll)
    seg_q = seg_v[me]
    qcp.wait()
    zero = jnp.zeros((64, T), BF)
    ones = jnp.ones((16, T), BF)

    def block(i, _):
        slot = lax.rem(i, KVS)
        blk = me - i

        @pl.when(i + 2 < count)
        def _():
            for c in kv_copies(blk - 2, lax.rem(i + 2, KVS)):
                c.start()

        @pl.when(i < RING)
        def _():
            start_weights(i, i)

        plain = (i > 0) & (seg_s[blk, 0, 0] == seg_s[blk, 0, T - 1])

        @pl.when(jnp.logical_not(plain))
        def _():
            seg_k = jnp.broadcast_to(seg_v[blk], (T, T)).T
            key = lax.broadcasted_iota(jnp.int32, (T, T), 0) - i * T
            qry = lax.broadcasted_iota(jnp.int32, (T, T), 1)
            bias[...] = jnp.where((seg_k == seg_q) & (key <= qry), 0.0, NEG)

        for c in kv_copies(blk, slot):
            c.wait()

        pl.when(plain)(lambda: attend(slot, seg_q == seg_s[blk, 0, 0]))
        pl.when(jnp.logical_not(plain))(lambda: attend(slot, None))
        return 0

    def attend(slot, seen):
        def score_dots(g):
            kg = jnp.concatenate([kb[slot, 0, g], kb[slot, 1, g]], axis=0)
            res = []
            for j in range(4):
                qj = qv[g, j * 64:(j + 1) * 64, :]
                qw = jnp.concatenate([zero] * j + [qj] + [zero] * (3 - j), axis=0)
                res.append(jnp.dot(kg, qw, preferred_element_type=F32))
            return res

        def score_store(res, par):
            for j in range(4):
                s = res[j] + bias[...] if seen is None else res[j]
                work[par * 4 + j] = s
                mx[par * 4 + j] = jnp.max(s, axis=0, keepdims=True)

        def soft(g, par):
            outs = []
            for j in range(4):
                head = g * 4 + j
                hs = slice(j * 64, (j + 1) * 64)
                m_old = mm[head]
                m_new = jnp.maximum(m_old, mx[par * 4 + j])
                if seen is None:
                    mc = m_new * scale
                    sub = mc
                else:
                    m_new = jnp.where(seen, m_new, m_old)
                    mc = m_new * scale
                    sub = jnp.where(seen, mc, -NEG)
                p = jnp.exp2(work[par * 4 + j] * scale - sub).astype(BF)
                alpha = jnp.exp2(m_old * scale - mc)
                vh = jnp.concatenate([vb[slot, 0, g, hs, :], vb[slot, 1, g, hs, :]], axis=1)
                o = jnp.dot(jnp.concatenate([vh, ones], axis=0), p, preferred_element_type=F32)
                outs.append((m_new, alpha, o))
            return outs

        def finish(g, outs):
            for j in range(4):
                head = g * 4 + j
                m_new, alpha, o = outs[j]
                mm[head] = m_new
                ll[head] = ll[head] * alpha + o[64:65, :]
                acc[head] = acc[head] * alpha + o[:64, :]

        score_store(score_dots(0), 0)

        def pair(i2, _):
            g = i2 * 2
            nxt = score_dots(g + 1)
            outs = soft(g, 0)
            score_store(nxt, 1)
            nxt = score_dots(g + 2)
            finish(g, outs)
            outs = soft(g + 1, 1)
            score_store(nxt, 0)
            finish(g + 1, outs)
            return 0

        lax.fori_loop(0, G // 2 - 1, pair, 0)
        nxt = score_dots(G - 1)
        outs = soft(G - 2, 0)
        score_store(nxt, 1)
        finish(G - 2, outs)
        finish(G - 1, soft(G - 1, 1))

    lax.fori_loop(0, count, block, 0)
    for t in range(1, RING):
        pl.when(t >= count)(functools.partial(start_weights, t, t))

    for g in range(G):
        parts = [acc[g * 4 + j] / ll[g * 4 + j] for j in range(4)]
        ot = jnp.concatenate(parts, axis=0)
        ob[:, g * 256:(g + 1) * 256] = ot.T.astype(BF)

    wocp.wait()
    hcp.wait()

    def proj(n, _):
        sl = pl.ds(pl.multiple_of(n * 512, 512), 512)
        r = jnp.dot(ob[...], wo_v[:, sl], preferred_element_type=F32).astype(BF)
        hb[:, sl] = hb[:, sl] + r
        return 0

    lax.fori_loop(0, D // 512, proj, 0)
    norm_rows(hb, gmlp, um, T)
    work[...] = jnp.zeros_like(work)

    def front(slot):
        a = jnp.dot(um[...], wg_v[slot], preferred_element_type=F32)
        b = jnp.dot(um[...], wu_v[slot], preferred_element_type=F32)
        return a, b

    def gate(a, b):
        a = a.astype(BF).astype(F32)
        b = b.astype(BF).astype(F32)
        return (jax.nn.silu(a) * b).astype(BF)

    def back(c, slot):
        for n in range(D // 256):
            work[n] += jnp.dot(c, wd_v[slot, :, n * 256:(n + 1) * 256], preferred_element_type=F32)

    for c in front_copies(0, 0):
        c.wait()
    cb[0] = gate(*front(0))

    def mlp(t, _):
        slot = lax.rem(t, RING)
        prev = lax.rem(t - 1, RING)
        for c in front_copies(t, slot):
            c.wait()
        back_copy(t - 1, prev).wait()
        a, b = front(slot)
        back(cb[lax.rem(t - 1, 2)], prev)
        cb[lax.rem(t, 2)] = gate(a, b)

        @pl.when(t - 1 + RING < steps)
        def _():
            start_weights(t - 1 + RING, prev)
        return 0

    lax.fori_loop(1, steps, mlp, 0)
    last = (steps - 1) % RING
    back_copy(steps - 1, last).wait()
    c = cb[(steps - 1) % 2]
    for n in range(D // 256):
        sl = slice(n * 256, (n + 1) * 256)
        y = work[n] + jnp.dot(c, wd_v[last, :, sl], preferred_element_type=F32)
        ob[:, sl] = hb[:, sl] + y.astype(BF)
        pltpu.make_async_copy(ob.at[:, sl], out.at[:, sl], o_sem.at[n]).start()
    for n in range(D // 256):
        sl = slice(n * 256, (n + 1) * 256)
        pltpu.make_async_copy(ob.at[:, sl], out.at[:, sl], o_sem.at[n]).wait()


def solution(mesh):
    ANY = pl.BlockSpec(memory_space=pl.ANY)
    VM = pl.BlockSpec(memory_space=pltpu.VMEM)
    SM = pl.BlockSpec(memory_space=pltpu.SMEM)
    DMA = pltpu.SemaphoreType.DMA

    def body(hidden, seg_ids, norm_kv, w_key, w_value, norm_attn, w_query, w_out, norm_mlp, w_gate, w_up, w_down):
        wk = w_key.transpose(1, 2, 0).reshape(D, D)
        wv = w_value.transpose(1, 2, 0).reshape(D, D)
        wq = w_query[0].transpose(1, 2, 0).reshape(D, D)
        seg = seg_ids.reshape(1, T)
        k_tiles = jax.ShapeDtypeStruct((16, G, T // 2, 256), BF)
        v_tiles = jax.ShapeDtypeStruct((16, G, 256, T // 2), BF)
        k4, v4, qt, seg_all = pl.pallas_call(
            gather_kernel,
            out_shape=(k_tiles, v_tiles, jax.ShapeDtypeStruct((G, 256, 256), BF), jax.ShapeDtypeStruct((8, 1, T), jnp.int32)),
            in_specs=[ANY, ANY, VM, VM, ANY, ANY, ANY],
            out_specs=(ANY, ANY, ANY, ANY),
            scratch_shapes=[
                pltpu.VMEM((4, T, D), BF), pltpu.VMEM((D, D), BF), pltpu.VMEM((D, D), BF), pltpu.VMEM((D, D), BF),
                pltpu.VMEM((T, D), BF), pltpu.VMEM((4, 2, G, T // 2, 256), BF), pltpu.VMEM((4, 2, G, 256, T // 2), BF),
                pltpu.VMEM((G, 256, 256), BF),
                DMA((3,)), DMA, DMA((4,)), DMA((4,)), DMA((4,)), DMA((4,)), DMA((4,)), DMA((4,)),
                DMA((7,)), DMA((7,)), DMA,
                DMA((4, 2)), DMA((4, G // 2, 2)), DMA((4, G // 2, 2)), DMA((4, 2)), DMA((4, G // 2, 2)), DMA((4, G // 2, 2)), DMA,
            ],
            compiler_params=pltpu.CompilerParams(collective_id=0, has_side_effects=True, vmem_limit_bytes=58 * 2 ** 20),
            cost_estimate=pl.CostEstimate(flops=20 * 10 ** 9, bytes_accessed=50 * 10 ** 6, transcendentals=0),
            name="gather_kv",
        )(hidden, seg, norm_kv, norm_attn, wk, wv, wq)

        return pl.pallas_call(
            layer_kernel,
            out_shape=jax.ShapeDtypeStruct((T, D), BF),
            in_specs=[SM, ANY, ANY, ANY, VM, ANY, VM, ANY, ANY, ANY, ANY],
            out_specs=ANY,
            scratch_shapes=[
                pltpu.VMEM((G, 256, 256), BF), pltpu.VMEM((KVS, 2, G, T // 2, 256), BF), pltpu.VMEM((KVS, 2, G, 256, T // 2), BF),
                pltpu.VMEM((T, T), F32), pltpu.VMEM((32, 64, T), F32), pltpu.VMEM((32, 1, T), F32), pltpu.VMEM((32, 1, T), F32), pltpu.VMEM((8, 1, T), F32),
                pltpu.VMEM((T, D), BF), pltpu.VMEM((T, D), BF), pltpu.VMEM((T, D), BF),
                pltpu.VMEM((D, D), BF), pltpu.VMEM((RING, D, FT), BF), pltpu.VMEM((RING, D, FT), BF), pltpu.VMEM((RING, FT, D), BF),
                pltpu.VMEM((2, T, FT), BF), pltpu.VMEM((8, T, 256), F32),
                DMA, DMA((KVS, 2)), DMA, DMA((RING, 3)), DMA, DMA((D // 256,)),
            ],
            compiler_params=pltpu.CompilerParams(vmem_limit_bytes=63 * 2 ** 20),
            cost_estimate=pl.CostEstimate(flops=40 * 10 ** 9, bytes_accessed=130 * 10 ** 6, transcendentals=10 ** 7),
            name="layer",
        )(seg_all, qt, k4, v4, seg_all, hidden, norm_mlp, w_out[0].reshape(D, D), w_gate[0], w_up[0], w_down[0])

    row_spec = P(('dp', 'sp'), None)
    in_specs = (row_spec, P(('dp', 'sp'))) + (P(),) * 10
    return jax.shard_map(body, mesh=mesh, in_specs=in_specs, out_specs=row_spec, check_vma=False)
```

```python
import functools
import math
import jax
import jax.numpy as jnp
from jax import lax
from jax.experimental import pallas as pl
from jax.experimental.pallas import tpu as pltpu
from jax.sharding import PartitionSpec as P

NORM_EPS = 1e-6
MESH = pl.DeviceIdType.MESH
BF = jnp.bfloat16
F32 = jnp.float32
NEG = -1e30
T = 256
D = 2048
G = 8
FT = 512
KVS = 3
RING = 6


def nt_dot(a, b):
    return lax.dot_general(a, b, (((1,), (1,)), ((), ())), preferred_element_type=F32)


def norm_rows(x_ref, gain_ref, out_ref, rows, start=0, step=16):
    gain = gain_ref[...].astype(F32)

    def body(i, _):
        sl = pl.ds(pl.multiple_of(start + i * step, step), step)
        x = x_ref[sl, :].astype(F32)
        inv = lax.rsqrt(jnp.mean(x * x, axis=-1, keepdims=True) + NORM_EPS)
        out_ref[sl, :] = (x * inv * gain).astype(BF)
        return 0

    lax.fori_loop(0, rows // step, body, 0, unroll=4)


def gather_kernel(hid, seg, gkv, gat, wk, wv, wq, k_out, v_out, q_out, seg_out,
                  hx, wk_v, wv_v, wq_v, wv_n, u, kst, vst, qst,
                  w_sem, own_sem, xs, xr, ys, yr, fs, fr, seg_s, seg_r, seg_l,
                  kl, ks, kr, vl, vs, vr, q_sem):
    me = lax.axis_index("sp")
    core = lax.rem(me, 2)
    xx = lax.rem(lax.div(me, 2), 2)
    yy = lax.div(me, 4)
    sib = me + 1 - 2 * core
    xp = me + 2 - 4 * xx
    yp = me + 4 - 8 * yy
    dg = xp + 4 - 8 * yy

    barrier = pltpu.get_barrier_semaphore()
    for d in range(1, 8):
        pl.semaphore_signal(barrier, inc=1, device_id={"sp": lax.rem(me + d, 8)}, device_id_type=MESH)
    own = pltpu.make_async_copy(hid, hx.at[0], own_sem)
    own.start()
    w_cp = [pltpu.make_async_copy(s, d, w_sem.at[i]) for i, (s, d) in enumerate(((wq, wq_v), (wk, wk_v), (wv, wv_v)))]
    for c in w_cp:
        c.start()
    seg_own = pltpu.make_async_copy(seg, seg_out.at[me], seg_l)
    seg_own.start()
    pl.semaphore_wait(barrier, 7)

    def send(src, dst, ss, rs, dev):
        return pltpu.make_async_remote_copy(src_ref=src, dst_ref=dst, send_sem=ss, recv_sem=rs,
                                            device_id={"sp": dev}, device_id_type=MESH)

    q4, half = T // 4, T // 2
    xcp, ycp = [], []
    for i in range(4):
        r = pl.ds(i * q4, q4)
        xcp.append(send(hid.at[r], hx.at[1 + i // 2, pl.ds((i % 2) * q4, q4)], xs.at[i], xr.at[i], xp))
        ycp.append(send(hid.at[r], hx.at[1 + i // 2, pl.ds(half + (i % 2) * q4, q4)], ys.at[i], yr.at[i], yp))
        xcp[-1].start()
        ycp[-1].start()
    segcp = []
    for d in range(1, 8):
        segcp.append(send(seg, seg_out.at[me], seg_s.at[d - 1], seg_r.at[d - 1], lax.rem(me + d, 8)))
        segcp[-1].start()

    own.wait()
    norm_rows(hx.at[0], gat, u, T)
    w_cp[0].wait()

    def q_body(g, _):
        for k in range(2):
            sl = pl.ds(pl.multiple_of(g * 512 + k * 256, 256), 256)
            qst[2 * g + k] = nt_dot(wq_v[sl, :], u[...]).astype(BF)
        return 0

    lax.fori_loop(0, G // 2, q_body, 0)
    qcp = pltpu.make_async_copy(qst, q_out, q_sem)
    qcp.start()

    def to_sibling(slot, st, parts, halves=(0, 1)):
        res = []
        for h in halves:
            gs = pl.ds(st * 2, 2)
            res.append(send(kst.at[slot, h, gs], k_out.at[parts[h], gs], ks.at[slot, st, h], kr.at[slot, st, h], sib))
            res.append(send(vst.at[slot, h, gs], v_out.at[parts[h], gs], vs.at[slot, st, h], vr.at[slot, st, h], sib))
        return res

    def to_self(slot, parts):
        res = []
        for h in range(2):
            res.append(pltpu.make_async_copy(kst.at[slot, h], k_out.at[parts[h]], kl.at[slot, h]))
            res.append(pltpu.make_async_copy(vst.at[slot, h], v_out.at[parts[h]], vl.at[slot, h]))
        return res

    def make_kv(slot, parts):
        def body(st, _):
            @pl.when(st > 0)
            def _():
                for c in to_sibling(slot, st - 1, parts):
                    c.start()

            for k in range(2):
                g = st * 2 + k
                sl = pl.ds(pl.multiple_of(g * 256, 256), 256)
                kk = nt_dot(u[...], wk_v[sl, :]).astype(BF)
                vv = nt_dot(wv_v[sl, :], u[...]).astype(BF)
                for h in range(2):
                    kst[slot, h, g] = kk[h * half:(h + 1) * half, :]
                    vst[slot, h, g] = vv[:, h * half:(h + 1) * half]
            return 0

        lax.fori_loop(0, G // 2, body, 0)
        for c in to_sibling(slot, G // 2 - 1, parts) + to_self(slot, parts):
            c.start()

    def flip(src, dst):
        def body(i, _):
            r = pl.ds(pl.multiple_of(i * 256, 256), 256)
            for j in range(D // 256):
                dst[j * 256:(j + 1) * 256, r] = src[r, j * 256:(j + 1) * 256].T
            return 0

        lax.fori_loop(0, D // 256, body, 0)

    def make_half(slot, h, parts):
        rows = slice(h * half, (h + 1) * half)

        def body(st, _):
            @pl.when(st > 0)
            def _():
                for c in to_sibling(slot, st - 1, parts, (h,)):
                    c.start()

            sl = pl.ds(pl.multiple_of(st * 512, 512), 512)
            kk = jnp.dot(u[rows, :], wq_v[:, sl], preferred_element_type=F32).astype(BF)
            vv = jnp.dot(u[rows, :], wv_n[:, sl], preferred_element_type=F32).T.astype(BF)
            for k in range(2):
                kst[slot, h, st * 2 + k] = kk[:, k * 256:(k + 1) * 256]
                vst[slot, h, st * 2 + k] = vv[k * 256:(k + 1) * 256, :]
            return 0

        lax.fori_loop(0, G // 2, body, 0)
        for c in to_sibling(slot, G // 2 - 1, parts, (h,)):
            c.start()

    norm_rows(hx.at[0], gkv, u, T)
    w_cp[1].wait()
    w_cp[2].wait()
    make_kv(0, (2 * me, 2 * me + 1))

    def forward(i):
        if i % 2 == 0:
            xcp[i].wait_recv()
            src, dev = hx.at[1 + i // 2, pl.ds(0, q4)], yp
        else:
            ycp[i].wait_recv()
            src, dev = hx.at[1 + i // 2, pl.ds(half + q4, q4)], xp
        c = send(src, hx.at[3, pl.ds(i * q4, q4)], fs.at[i], fr.at[i], dev)
        c.start()
        return c

    fcp = [forward(0), forward(1)]
    xcp[1].wait_recv()
    ycp[0].wait_recv()
    norm_rows(hx.at[1], gkv, u, T)
    make_kv(1, (2 * xp, 2 * yp))
    fcp.append(forward(2))
    flip(wk_v, wq_v)
    flip(wv_v, wv_n)
    fcp.append(forward(3))
    xcp[3].wait_recv()
    ycp[2].wait_recv()
    norm_rows(hx.at[2], gkv, u, T)
    make_kv(2, (2 * xp + 1, 2 * yp + 1))
    fcp[0].wait_recv()
    fcp[1].wait_recv()
    last = (2 * dg, 2 * dg + 1)
    norm_rows(hx.at[3], gkv, u, half)
    make_half(3, 0, last)
    fcp[2].wait_recv()
    fcp[3].wait_recv()
    norm_rows(hx.at[3], gkv, u, half, half)
    make_half(3, 1, last)
    for c in to_self(3, last):
        c.start()

    qcp.wait()
    seg_own.wait()
    for c in segcp:
        c.wait()
    for c in xcp + ycp + fcp:
        c.wait_send()

    def drain(i, _):
        slot, st = lax.div(i, G // 2), lax.rem(i, G // 2)
        for c in to_sibling(slot, st, (2 * me, 2 * me + 1)):
            c.wait()
        return 0

    lax.fori_loop(0, 4 * (G // 2), drain, 0)
    for slot in range(4):
        for c in to_self(slot, (2 * me, 2 * me + 1)):
            c.wait()


def layer_kernel(seg_s, qt, k4, v4, seg_v, hid, gmlp, wo, wg, wu, wd, out,
                 qv, kb, vb, bias, acc, mm, ll, mx, ob, hb, um, wo_v, wg_v, wu_v, wd_v, cb, work,
                 q_sem, kv_sem, wo_sem, w_sem, h_sem, o_sem):
    me = lax.axis_index("sp")
    steps = wg.shape[1] // FT
    scale = (64 ** -0.5) * math.log2(math.e)

    def kv_copies(blk, slot):
        two = pl.ds(2 * blk, 2)
        return (pltpu.make_async_copy(k4.at[two], kb.at[slot], kv_sem.at[slot, 0]),
                pltpu.make_async_copy(v4.at[two], vb.at[slot], kv_sem.at[slot, 1]))

    def front_copies(t, slot):
        sl = pl.ds(pl.multiple_of(t * FT, FT), FT)
        return (pltpu.make_async_copy(wg.at[:, sl], wg_v.at[slot], w_sem.at[slot, 0]),
                pltpu.make_async_copy(wu.at[:, sl], wu_v.at[slot], w_sem.at[slot, 1]))

    def back_copy(t, slot):
        sl = pl.ds(pl.multiple_of(t * FT, FT), FT)
        return pltpu.make_async_copy(wd.at[sl, :], wd_v.at[slot], w_sem.at[slot, 2])

    def start_weights(t, slot):
        for c in front_copies(t, slot):
            c.start(priority=1)
        back_copy(t, slot).start(priority=1)

    qcp = pltpu.make_async_copy(qt, qv, q_sem)
    qcp.start()
    for c in kv_copies(me, 0):
        c.start()
    hcp = pltpu.make_async_copy(hid, hb, h_sem)
    hcp.start()

    first = seg_s[me, 0, 0]
    low = jnp.int32(0)
    for b in range(8):
        low = low + jnp.where((b < me) & (seg_s[b, 0, T - 1] < first), 1, 0).astype(jnp.int32)
    count = me - low + 1

    @pl.when(count > 1)
    def _():
        for c in kv_copies(me - 1, 1):
            c.start()

    wocp = pltpu.make_async_copy(wo, wo_v, wo_sem)
    wocp.start(priority=1)

    acc[...] = jnp.zeros_like(acc)
    mm[...] = jnp.full_like(mm, NEG)
    ll[...] = jnp.zeros_like(ll)
    seg_q = seg_v[me]
    qcp.wait()
    zero = jnp.zeros((64, T), BF)
    ones = jnp.ones((16, T), BF)

    def block(i, _):
        slot = lax.rem(i, KVS)
        blk = me - i

        @pl.when(i + 2 < count)
        def _():
            for c in kv_copies(blk - 2, lax.rem(i + 2, KVS)):
                c.start()

        @pl.when(i < RING)
        def _():
            start_weights(i, i)

        plain = (i > 0) & (seg_s[blk, 0, 0] == seg_s[blk, 0, T - 1])

        @pl.when(jnp.logical_not(plain))
        def _():
            seg_k = jnp.broadcast_to(seg_v[blk], (T, T)).T
            key = lax.broadcasted_iota(jnp.int32, (T, T), 0) - i * T
            qry = lax.broadcasted_iota(jnp.int32, (T, T), 1)
            bias[...] = jnp.where((seg_k == seg_q) & (key <= qry), 0.0, NEG)

        for c in kv_copies(blk, slot):
            c.wait()

        pl.when(plain)(lambda: attend(slot, seg_q == seg_s[blk, 0, 0]))
        pl.when(jnp.logical_not(plain))(lambda: attend(slot, None))
        return 0

    def attend(slot, seen):
        def score_dots(g):
            kg = jnp.concatenate([kb[slot, 0, g], kb[slot, 1, g]], axis=0)
            res = []
            for j in range(4):
                qj = qv[g, j * 64:(j + 1) * 64, :]
                qw = jnp.concatenate([zero] * j + [qj] + [zero] * (3 - j), axis=0)
                res.append(jnp.dot(kg, qw, preferred_element_type=F32))
            return res

        def score_store(res, par):
            for j in range(4):
                s = res[j] + bias[...] if seen is None else res[j]
                work[par * 4 + j] = s
                mx[par * 4 + j] = jnp.max(s, axis=0, keepdims=True)

        def soft(g, par):
            outs = []
            for j in range(4):
                head = g * 4 + j
                hs = slice(j * 64, (j + 1) * 64)
                m_old = mm[head]
                m_new = jnp.maximum(m_old, mx[par * 4 + j])
                if seen is None:
                    mc = m_new * scale
                    sub = mc
                else:
                    m_new = jnp.where(seen, m_new, m_old)
                    mc = m_new * scale
                    sub = jnp.where(seen, mc, -NEG)
                p = jnp.exp2(work[par * 4 + j] * scale - sub).astype(BF)
                alpha = jnp.exp2(m_old * scale - mc)
                vh = jnp.concatenate([vb[slot, 0, g, hs, :], vb[slot, 1, g, hs, :]], axis=1)
                o = jnp.dot(jnp.concatenate([vh, ones], axis=0), p, preferred_element_type=F32)
                outs.append((m_new, alpha, o))
            return outs

        def finish(g, outs):
            for j in range(4):
                head = g * 4 + j
                m_new, alpha, o = outs[j]
                mm[head] = m_new
                ll[head] = ll[head] * alpha + o[64:65, :]
                acc[head] = acc[head] * alpha + o[:64, :]

        score_store(score_dots(0), 0)

        def pair(i2, _):
            g = i2 * 2
            nxt = score_dots(g + 1)
            outs = soft(g, 0)
            score_store(nxt, 1)
            nxt = score_dots(g + 2)
            finish(g, outs)
            outs = soft(g + 1, 1)
            score_store(nxt, 0)
            finish(g + 1, outs)
            return 0

        lax.fori_loop(0, G // 2 - 1, pair, 0)
        nxt = score_dots(G - 1)
        outs = soft(G - 2, 0)
        score_store(nxt, 1)
        finish(G - 2, outs)
        finish(G - 1, soft(G - 1, 1))

    lax.fori_loop(0, count, block, 0)
    for t in range(1, RING):
        pl.when(t >= count)(functools.partial(start_weights, t, t))

    for g in range(G):
        parts = [acc[g * 4 + j] / ll[g * 4 + j] for j in range(4)]
        ot = jnp.concatenate(parts, axis=0)
        ob[:, g * 256:(g + 1) * 256] = ot.T.astype(BF)

    wocp.wait()
    hcp.wait()

    def proj(n, _):
        sl = pl.ds(pl.multiple_of(n * 512, 512), 512)
        r = jnp.dot(ob[...], wo_v[:, sl], preferred_element_type=F32).astype(BF)
        hb[:, sl] = hb[:, sl] + r
        return 0

    lax.fori_loop(0, D // 512, proj, 0)
    norm_rows(hb, gmlp, um, T)
    work[...] = jnp.zeros_like(work)

    def front(slot):
        a = jnp.dot(um[...], wg_v[slot], preferred_element_type=F32)
        b = jnp.dot(um[...], wu_v[slot], preferred_element_type=F32)
        return a, b

    def gate(a, b):
        a = a.astype(BF).astype(F32)
        b = b.astype(BF).astype(F32)
        return (jax.nn.silu(a) * b).astype(BF)

    def back(c, slot):
        for n in range(D // 256):
            work[n] += jnp.dot(c, wd_v[slot, :, n * 256:(n + 1) * 256], preferred_element_type=F32)

    for c in front_copies(0, 0):
        c.wait()
    cb[0] = gate(*front(0))

    def mlp(t, _):
        slot = lax.rem(t, RING)
        prev = lax.rem(t - 1, RING)
        for c in front_copies(t, slot):
            c.wait()
        back_copy(t - 1, prev).wait()
        a, b = front(slot)
        back(cb[lax.rem(t - 1, 2)], prev)
        cb[lax.rem(t, 2)] = gate(a, b)

        @pl.when(t - 1 + RING < steps)
        def _():
            start_weights(t - 1 + RING, prev)
        return 0

    def mlp2(i, _):
        t = 2 * i + 1
        s0, s1, s2 = lax.rem(t - 1, RING), lax.rem(t, RING), lax.rem(t + 1, RING)
        for c in front_copies(t, s1) + front_copies(t + 1, s2):
            c.wait()
        back_copy(t - 1, s0).wait()
        back_copy(t, s1).wait()
        a, b = front(s1)
        back(cb[0], s0)
        c1 = gate(a, b)
        a, b = front(s2)
        back(c1, s1)
        cb[0] = gate(a, b)
        for k, s in ((0, s0), (1, s1)):
            @pl.when(t - 1 + k + RING < steps)
            def _():
                start_weights(t - 1 + k + RING, s)
        return 0

    lax.fori_loop(0, (steps - 2) // 2, mlp2, 0)
    t = steps - 1
    for c in front_copies(t, t % RING):
        c.wait()
    back_copy(t - 1, (t - 1) % RING).wait()
    a, b = front(t % RING)
    back(cb[0], (t - 1) % RING)
    cb[1] = gate(a, b)
    last = (steps - 1) % RING
    back_copy(steps - 1, last).wait()
    c = cb[(steps - 1) % 2]
    for n in range(D // 256):
        sl = slice(n * 256, (n + 1) * 256)
        y = work[n] + jnp.dot(c, wd_v[last, :, sl], preferred_element_type=F32)
        ob[:, sl] = hb[:, sl] + y.astype(BF)
        pltpu.make_async_copy(ob.at[:, sl], out.at[:, sl], o_sem.at[n]).start()
    for n in range(D // 256):
        sl = slice(n * 256, (n + 1) * 256)
        pltpu.make_async_copy(ob.at[:, sl], out.at[:, sl], o_sem.at[n]).wait()


def solution(mesh):
    ANY = pl.BlockSpec(memory_space=pl.ANY)
    VM = pl.BlockSpec(memory_space=pltpu.VMEM)
    SM = pl.BlockSpec(memory_space=pltpu.SMEM)
    DMA = pltpu.SemaphoreType.DMA

    def body(hidden, seg_ids, norm_kv, w_key, w_value, norm_attn, w_query, w_out, norm_mlp, w_gate, w_up, w_down):
        wk = w_key.transpose(1, 2, 0).reshape(D, D)
        wv = w_value.transpose(1, 2, 0).reshape(D, D)
        wq = w_query[0].transpose(1, 2, 0).reshape(D, D)
        seg = seg_ids.reshape(1, T)
        k_tiles = jax.ShapeDtypeStruct((16, G, T // 2, 256), BF)
        v_tiles = jax.ShapeDtypeStruct((16, G, 256, T // 2), BF)
        k4, v4, qt, seg_all = pl.pallas_call(
            gather_kernel,
            out_shape=(k_tiles, v_tiles, jax.ShapeDtypeStruct((G, 256, 256), BF), jax.ShapeDtypeStruct((8, 1, T), jnp.int32)),
            in_specs=[ANY, ANY, VM, VM, ANY, ANY, ANY],
            out_specs=(ANY, ANY, ANY, ANY),
            scratch_shapes=[
                pltpu.VMEM((4, T, D), BF), pltpu.VMEM((D, D), BF), pltpu.VMEM((D, D), BF), pltpu.VMEM((D, D), BF), pltpu.VMEM((D, D), BF),
                pltpu.VMEM((T, D), BF), pltpu.VMEM((4, 2, G, T // 2, 256), BF), pltpu.VMEM((4, 2, G, 256, T // 2), BF),
                pltpu.VMEM((G, 256, 256), BF),
                DMA((3,)), DMA, DMA((4,)), DMA((4,)), DMA((4,)), DMA((4,)), DMA((4,)), DMA((4,)),
                DMA((7,)), DMA((7,)), DMA,
                DMA((4, 2)), DMA((4, G // 2, 2)), DMA((4, G // 2, 2)), DMA((4, 2)), DMA((4, G // 2, 2)), DMA((4, G // 2, 2)), DMA,
            ],
            compiler_params=pltpu.CompilerParams(collective_id=0, has_side_effects=True, vmem_limit_bytes=60 * 2 ** 20),
            cost_estimate=pl.CostEstimate(flops=20 * 10 ** 9, bytes_accessed=50 * 10 ** 6, transcendentals=0),
            name="gather_kv",
        )(hidden, seg, norm_kv, norm_attn, wk, wv, wq)

        return pl.pallas_call(
            layer_kernel,
            out_shape=jax.ShapeDtypeStruct((T, D), BF),
            in_specs=[SM, ANY, ANY, ANY, VM, ANY, VM, ANY, ANY, ANY, ANY],
            out_specs=ANY,
            scratch_shapes=[
                pltpu.VMEM((G, 256, 256), BF), pltpu.VMEM((KVS, 2, G, T // 2, 256), BF), pltpu.VMEM((KVS, 2, G, 256, T // 2), BF),
                pltpu.VMEM((T, T), F32), pltpu.VMEM((32, 64, T), F32), pltpu.VMEM((32, 1, T), F32), pltpu.VMEM((32, 1, T), F32), pltpu.VMEM((8, 1, T), F32),
                pltpu.VMEM((T, D), BF), pltpu.VMEM((T, D), BF), pltpu.VMEM((T, D), BF),
                pltpu.VMEM((D, D), BF), pltpu.VMEM((RING, D, FT), BF), pltpu.VMEM((RING, D, FT), BF), pltpu.VMEM((RING, FT, D), BF),
                pltpu.VMEM((2, T, FT), BF), pltpu.VMEM((8, T, 256), F32),
                DMA, DMA((KVS, 2)), DMA, DMA((RING, 3)), DMA, DMA((D // 256,)),
            ],
            compiler_params=pltpu.CompilerParams(vmem_limit_bytes=63 * 2 ** 20),
            cost_estimate=pl.CostEstimate(flops=40 * 10 ** 9, bytes_accessed=130 * 10 ** 6, transcendentals=10 ** 7),
            name="layer",
        )(seg_all, qt, k4, v4, seg_all, hidden, norm_mlp, w_out[0].reshape(D, D), w_gate[0], w_up[0], w_down[0])

    row_spec = P(('dp', 'sp'), None)
    in_specs = (row_spec, P(('dp', 'sp'))) + (P(),) * 10
    return jax.shard_map(body, mesh=mesh, in_specs=in_specs, out_specs=row_spec, check_vma=False)
```

```python
import functools
import math
import jax
import jax.numpy as jnp
from jax import lax
from jax.experimental import pallas as pl
from jax.experimental.pallas import tpu as pltpu
from jax.sharding import PartitionSpec as P

NORM_EPS = 1e-6
MESH = pl.DeviceIdType.MESH
BF = jnp.bfloat16
F32 = jnp.float32
NEG = -1e30
T = 256
W = 256
H = 128
HD = 64
D = 2048
G = 8
GP = 4
DN = 8
FT = 512
KVS = 3
RING = 6


def nt_dot(a, b):
    return lax.dot_general(a, b, (((1,), (1,)), ((), ())), preferred_element_type=F32)


def norm_rows(x_ref, gain_ref, out_ref, rows, start=0, step=16):
    gain = gain_ref[...].astype(F32)

    def body(i, _):
        sl = pl.ds(pl.multiple_of(start + i * step, step), step)
        x = x_ref[sl, :].astype(F32)
        inv = lax.rsqrt(jnp.mean(x * x, axis=-1, keepdims=True) + NORM_EPS)
        out_ref[sl, :] = (x * inv * gain).astype(BF)
        return 0

    lax.fori_loop(0, rows // step, body, 0, unroll=4)


class Attention:
    def __init__(self, kt, vt, qv, bias, work, mx, mm, ll, acc, seen):
        self.refs = kt, vt, qv, bias, work, mx, mm, ll, acc
        self.seen = seen
        self.scale = (HD ** -0.5) * math.log2(math.e)

    def dots(self, g):
        kt, _, qv = self.refs[:3]
        zero = jnp.zeros((HD, T), BF)
        kg = jnp.concatenate([kt[0, g], kt[1, g]], axis=0)
        res = []
        for j in range(4):
            qj = qv[g, j * HD:(j + 1) * HD, :]
            qw = jnp.concatenate([zero] * j + [qj] + [zero] * (3 - j), axis=0)
            res.append(jnp.dot(kg, qw, preferred_element_type=F32))
        return res

    def store(self, res, par):
        bias, work, mx = self.refs[3:6]
        for j in range(4):
            s = res[j] + bias[...] if self.seen is None else res[j]
            work[par * 4 + j] = s
            mx[par * 4 + j] = jnp.max(s, axis=0, keepdims=True)

    def soft(self, g, par):
        _, vt, _, _, work, mx, mm, _, _ = self.refs
        seen, scale = self.seen, self.scale
        ones = jnp.ones((16, T), BF)
        outs = []
        for j in range(4):
            head = g * 4 + j
            hs = slice(j * HD, (j + 1) * HD)
            m_old = mm[head]
            m_new = jnp.maximum(m_old, mx[par * 4 + j])
            if seen is None:
                mc = m_new * scale
                sub = mc
            else:
                m_new = jnp.where(seen, m_new, m_old)
                mc = m_new * scale
                sub = jnp.where(seen, mc, -NEG)
            p = jnp.exp2(work[par * 4 + j] * scale - sub).astype(BF)
            alpha = jnp.exp2(m_old * scale - mc)
            vh = jnp.concatenate([vt[0, g, hs, :], vt[1, g, hs, :]], axis=1)
            o = jnp.dot(jnp.concatenate([vh, ones], axis=0), p, preferred_element_type=F32)
            outs.append((m_new, alpha, o))
        return outs

    def finish(self, g, outs):
        mm, ll, acc = self.refs[6:]
        for j in range(4):
            head = g * 4 + j
            m_new, alpha, o = outs[j]
            mm[head] = m_new
            ll[head] = ll[head] * alpha + o[HD:65, :]
            acc[head] = acc[head] * alpha + o[:HD, :]

    def begin(self):
        self.store(self.dots(0), 0)

    def step(self, i2, following, between=lambda k: None):
        g = i2 * 2
        nxt = self.dots(g + 1)
        first = between(0)
        outs = self.soft(g, 0)
        self.store(nxt, 1)
        nxt = self.dots(following)
        second = between(1)
        self.finish(g, outs)
        outs = self.soft(g + 1, 1)
        self.store(nxt, 0)
        self.finish(g + 1, outs)
        return first, second

    def run(self):
        self.begin()

        def pair(i2, _):
            self.step(i2, i2 * 2 + 2)
            return 0

        lax.fori_loop(0, GP - 1, pair, 0)
        nxt = self.dots(G - 1)
        outs = self.soft(G - 2, 0)
        self.store(nxt, 1)
        self.finish(G - 2, outs)
        self.finish(G - 1, self.soft(G - 1, 1))


def gather_kernel(hid, seg, gkv, gat, wk, wv, wq, k_out, v_out, q_out, seg_out, acc_out, m_out, l_out,
                  hx, wk_v, wv_v, wq_v, wv_n, u, kst, vst, qst,
                  w_sem, own_sem, xs, xr, ys, yr, fs, fr, seg_s, seg_r, seg_l,
                  kl, ks, kr, vl, vs, vr, q_sem,
                  sk, sv, seg_v, bias, work, mx, mm, ll, acc, st_sem):
    me = lax.axis_index("sp")
    core = lax.rem(me, 2)
    xx = lax.rem(lax.div(me, 2), 2)
    yy = lax.div(me, 4)
    sib = me + 1 - 2 * core
    xp = me + 2 - 4 * xx
    yp = me + 4 - 8 * yy
    dg = xp + 4 - 8 * yy
    mine = (2 * me, 2 * me + 1)

    barrier = pltpu.get_barrier_semaphore()
    for d in range(1, 8):
        pl.semaphore_signal(barrier, inc=1, device_id={"sp": lax.rem(me + d, 8)}, device_id_type=MESH)
    own = pltpu.make_async_copy(hid, hx.at[0], own_sem)
    own.start()
    w_cp = [pltpu.make_async_copy(s, d, w_sem.at[i]) for i, (s, d) in enumerate(((wq, wq_v), (wk, wk_v), (wv, wv_v)))]
    for c in w_cp:
        c.start()
    seg_own = pltpu.make_async_copy(seg, seg_out.at[me], seg_l)
    seg_own.start()
    pl.semaphore_wait(barrier, 7)

    def send(src, dst, ss, rs, dev):
        return pltpu.make_async_remote_copy(src_ref=src, dst_ref=dst, send_sem=ss, recv_sem=rs,
                                            device_id={"sp": dev}, device_id_type=MESH)

    segcp = []
    for d in range(1, 8):
        segcp.append(send(seg, seg_out.at[me], seg_s.at[d - 1], seg_r.at[d - 1], lax.rem(me + d, 8)))
        segcp[-1].start()

    q4, half = T // 4, H
    xcp, ycp = [], []
    for i in range(4):
        r = pl.ds(i * q4, q4)
        xcp.append(send(hid.at[r], hx.at[1 + i // 2, pl.ds((i % 2) * q4, q4)], xs.at[i], xr.at[i], xp))
        ycp.append(send(hid.at[r], hx.at[1 + i // 2, pl.ds(half + (i % 2) * q4, q4)], ys.at[i], yr.at[i], yp))
        xcp[-1].start()
        ycp[-1].start()

    own.wait()
    norm_rows(hx.at[0], gat, u, T)
    w_cp[0].wait()

    def q_body(g, _):
        for k in range(2):
            sl = pl.ds(pl.multiple_of(g * 512 + k * W, W), W)
            qst[2 * g + k] = nt_dot(wq_v[sl, :], u[...]).astype(BF)
        return 0

    lax.fori_loop(0, GP, q_body, 0)
    qcp = pltpu.make_async_copy(qst, q_out, q_sem)
    qcp.start()

    def to_sibling(slot, st, parts, halves=(0, 1)):
        res = []
        for h in halves:
            gs = pl.ds(st * 2, 2)
            res.append(send(kst.at[slot, h, gs], k_out.at[parts[h], gs], ks.at[slot, st, h], kr.at[slot, st, h], sib))
            res.append(send(vst.at[slot, h, gs], v_out.at[parts[h], gs], vs.at[slot, st, h], vr.at[slot, st, h], sib))
        return res

    def to_self(slot, parts):
        res = []
        for h in range(2):
            res.append(pltpu.make_async_copy(kst.at[slot, h], k_out.at[parts[h]], kl.at[slot, h]))
            res.append(pltpu.make_async_copy(vst.at[slot, h], v_out.at[parts[h]], vl.at[slot, h]))
        return res

    def flip(src, dst, i):
        for k in range(2):
            r = pl.ds(pl.multiple_of(i * 512 + k * W, W), W)
            for j in range(DN):
                dst[j * W:(j + 1) * W, r] = src[r, j * W:(j + 1) * W].T

    def make_kv(slot, parts, att=None, turn=None):
        def body(st, _):
            @pl.when(st > 0)
            def _():
                for c in to_sibling(slot, st - 1, parts):
                    c.start()

            def products(k):
                sl = pl.ds(pl.multiple_of(st * 512 + k * W, W), W)
                return nt_dot(u[...], wk_v[sl, :]), nt_dot(wv_v[sl, :], u[...])

            if att is None:
                both = products(0), products(1)
            else:
                both = att.step(st, jnp.minimum(st * 2 + 2, G - 1), products)
                flip(*turn, st)
            for k in range(2):
                kk, vv = both[k][0].astype(BF), both[k][1].astype(BF)
                for h in range(2):
                    kst[slot, h, st * 2 + k] = kk[h * half:(h + 1) * half, :]
                    vst[slot, h, st * 2 + k] = vv[:, h * half:(h + 1) * half]
            return 0

        lax.fori_loop(0, GP, body, 0)
        for c in to_sibling(slot, GP - 1, parts) + to_self(slot, parts):
            c.start()

    def make_half(slot, h, parts):
        rows = slice(h * half, (h + 1) * half)

        def body(st, _):
            @pl.when(st > 0)
            def _():
                for c in to_sibling(slot, st - 1, parts, (h,)):
                    c.start()

            sl = pl.ds(pl.multiple_of(st * 512, 512), 512)
            kk = jnp.dot(u[rows, :], wq_v[:, sl], preferred_element_type=F32).astype(BF)
            vv = jnp.dot(u[rows, :], wv_n[:, sl], preferred_element_type=F32).T.astype(BF)
            for k in range(2):
                kst[slot, h, st * 2 + k] = kk[:, k * W:(k + 1) * W]
                vst[slot, h, st * 2 + k] = vv[k * W:(k + 1) * W, :]
            return 0

        lax.fori_loop(0, GP, body, 0)
        for c in to_sibling(slot, GP - 1, parts, (h,)):
            c.start()

    norm_rows(hx.at[0], gkv, u, T)
    w_cp[1].wait()
    w_cp[2].wait()
    make_kv(0, mine)

    acc[...] = jnp.zeros_like(acc)
    mm[...] = jnp.full_like(mm, NEG)
    ll[...] = jnp.zeros_like(ll)
    seg_own.wait()
    for c in segcp:
        c.wait()
    seg_cp = pltpu.make_async_copy(seg_out, seg_v, seg_l)
    seg_cp.start()
    seg_cp.wait()

    def attention(kt, vt, blk):
        seg_k = jnp.broadcast_to(seg_v[blk], (T, T)).T
        key = lax.broadcasted_iota(jnp.int32, (T, T), 0) + (blk - me) * T
        qry = lax.broadcasted_iota(jnp.int32, (T, T), 1)
        bias[...] = jnp.where((seg_k == seg_v[me]) & (key <= qry), 0.0, NEG)
        att = Attention(kt, vt, qst, bias, work, mx, mm, ll, acc, None)
        att.begin()
        return att

    def forward(i):
        if i % 2 == 0:
            xcp[i].wait_recv()
            src, dev = hx.at[1 + i // 2, pl.ds(0, q4)], yp
        else:
            ycp[i].wait_recv()
            src, dev = hx.at[1 + i // 2, pl.ds(half + q4, q4)], xp
        c = send(src, hx.at[3, pl.ds(i * q4, q4)], fs.at[i], fr.at[i], dev)
        c.start()
        return c

    fcp = [forward(0), forward(1)]

    def sib_recv(st, _):
        for c in to_sibling(0, st, mine):
            c.wait_recv()
        return 0

    lax.fori_loop(0, GP, sib_recv, 0)
    sib_cp = [pltpu.make_async_copy(k_out.at[pl.ds(2 * sib, 2)], sk, st_sem.at[0]),
              pltpu.make_async_copy(v_out.at[pl.ds(2 * sib, 2)], sv, st_sem.at[1])]
    for c in sib_cp:
        c.start()
    att = attention(kst.at[0], vst.at[0], me)
    xcp[1].wait_recv()
    ycp[0].wait_recv()
    norm_rows(hx.at[1], gkv, u, T)
    make_kv(1, (2 * xp, 2 * yp), att, (wk_v, wq_v))
    fcp.append(forward(2))
    fcp.append(forward(3))
    for c in sib_cp:
        c.wait()
    att = attention(sk, sv, sib)
    xcp[3].wait_recv()
    ycp[2].wait_recv()
    norm_rows(hx.at[2], gkv, u, T)
    make_kv(2, (2 * xp + 1, 2 * yp + 1), att, (wv_v, wv_n))
    state_cp = [pltpu.make_async_copy(a, b, st_sem.at[2 + i]) for i, (a, b) in enumerate(((acc, acc_out), (mm, m_out), (ll, l_out)))]
    for c in state_cp:
        c.start()
    fcp[0].wait_recv()
    fcp[1].wait_recv()
    last = (2 * dg, 2 * dg + 1)
    norm_rows(hx.at[3], gkv, u, half)
    make_half(3, 0, last)
    fcp[2].wait_recv()
    fcp[3].wait_recv()
    norm_rows(hx.at[3], gkv, u, half, half)
    make_half(3, 1, last)
    for c in to_self(3, last):
        c.start()

    qcp.wait()
    for c in state_cp:
        c.wait()
    for c in xcp + ycp + fcp:
        c.wait_send()

    def drain(i, _):
        slot, st = lax.div(i, GP), lax.rem(i, GP)
        for c in to_sibling(slot, st, mine):
            c.wait()
        return 0

    def sib_sent(st, _):
        for c in to_sibling(0, st, mine):
            c.wait_send()
        return 0

    lax.fori_loop(0, GP, sib_sent, 0)
    lax.fori_loop(GP, 4 * (GP), drain, 0)
    for slot in range(4):
        for c in to_self(slot, mine):
            c.wait()


def layer_kernel(seg_s, qt, k4, v4, acc_in, m_in, l_in, seg_v, hid, gmlp, wo, wg, wu, wd, out,
                 qv, kb, vb, bias, acc, mm, ll, mx, ob, hb, um, wo_v, wg_v, wu_v, wd_v, cb, work,
                 q_sem, kv_sem, wo_sem, w_sem, h_sem, o_sem, st_sem):
    me = lax.axis_index("sp")
    steps = wg.shape[1] // FT

    def kv_copies(blk, slot):
        two = pl.ds(2 * blk, 2)
        return (pltpu.make_async_copy(k4.at[two], kb.at[slot], kv_sem.at[slot, 0]),
                pltpu.make_async_copy(v4.at[two], vb.at[slot], kv_sem.at[slot, 1]))

    def front_copies(t, slot):
        sl = pl.ds(pl.multiple_of(t * FT, FT), FT)
        return (pltpu.make_async_copy(wg.at[:, sl], wg_v.at[slot], w_sem.at[slot, 0]),
                pltpu.make_async_copy(wu.at[:, sl], wu_v.at[slot], w_sem.at[slot, 1]))

    def back_copy(t, slot):
        sl = pl.ds(pl.multiple_of(t * FT, FT), FT)
        return pltpu.make_async_copy(wd.at[sl, :], wd_v.at[slot], w_sem.at[slot, 2])

    def start_weights(t, slot):
        for c in front_copies(t, slot):
            c.start(priority=1)
        back_copy(t, slot).start(priority=1)

    first = seg_s[me, 0, 0]
    low = jnp.int32(0)
    for b in range(8):
        low = low + jnp.where((b < me) & (seg_s[b, 0, T - 1] < first), 1, 0).astype(jnp.int32)
    top = me - 1 - lax.rem(me, 2)
    count = jnp.maximum(top - low + 1, 0)

    for n in range(2):
        @pl.when(n < count)
        def _():
            for c in kv_copies(top - n, n):
                c.start()

    qcp = pltpu.make_async_copy(qt, qv, q_sem)
    qcp.start()
    state = [pltpu.make_async_copy(a, b, st_sem.at[i]) for i, (a, b) in enumerate(((acc_in, acc), (m_in, mm), (l_in, ll)))]
    for c in state:
        c.start()
    hcp = pltpu.make_async_copy(hid, hb, h_sem)
    hcp.start()
    wocp = pltpu.make_async_copy(wo, wo_v, wo_sem)
    wocp.start(priority=1)
    seg_q = seg_v[me]
    qcp.wait()
    for c in state:
        c.wait()

    def block(i, _):
        slot = lax.rem(i, KVS)
        blk = top - i

        @pl.when(i + 2 < count)
        def _():
            for c in kv_copies(blk - 2, lax.rem(i + 2, KVS)):
                c.start()

        @pl.when(i < RING)
        def _():
            start_weights(i, i)

        plain = (seg_s[blk, 0, 0] == seg_s[blk, 0, T - 1])

        @pl.when(jnp.logical_not(plain))
        def _():
            seg_k = jnp.broadcast_to(seg_v[blk], (T, T)).T
            bias[...] = jnp.where(seg_k == seg_q, 0.0, NEG)

        for c in kv_copies(blk, slot):
            c.wait()

        run = lambda seen: Attention(kb.at[slot], vb.at[slot], qv, bias, work, mx, mm, ll, acc, seen).run()
        pl.when(plain)(lambda: run(seg_q == seg_s[blk, 0, 0]))
        pl.when(jnp.logical_not(plain))(lambda: run(None))
        return 0

    lax.fori_loop(0, count, block, 0)
    for t in range(RING):
        pl.when(t >= count)(functools.partial(start_weights, t, t))

    for g in range(G):
        parts = [acc[g * 4 + j] / ll[g * 4 + j] for j in range(4)]
        ot = jnp.concatenate(parts, axis=0)
        ob[:, g * W:(g + 1) * W] = ot.T.astype(BF)

    wocp.wait()
    hcp.wait()

    def proj(n, _):
        sl = pl.ds(pl.multiple_of(n * 512, 512), 512)
        r = jnp.dot(ob[...], wo_v[:, sl], preferred_element_type=F32).astype(BF)
        hb[:, sl] = hb[:, sl] + r
        return 0

    lax.fori_loop(0, D // 512, proj, 0, unroll=2)
    norm_rows(hb, gmlp, um, T)
    work[...] = jnp.zeros_like(work)

    def front(slot):
        a = jnp.dot(um[...], wg_v[slot], preferred_element_type=F32)
        b = jnp.dot(um[...], wu_v[slot], preferred_element_type=F32)
        return a, b

    def gate(a, b):
        a = a.astype(BF).astype(F32)
        b = b.astype(BF).astype(F32)
        return (jax.nn.silu(a) * b).astype(BF)

    def back(c, slot):
        for n in range(DN):
            work[n] += jnp.dot(c, wd_v[slot, :, n * W:(n + 1) * W], preferred_element_type=F32)

    for c in front_copies(0, 0):
        c.wait()
    cb[0] = gate(*front(0))

    def mlp(t, _):
        slot = lax.rem(t, RING)
        prev = lax.rem(t - 1, RING)
        for c in front_copies(t, slot):
            c.wait()
        back_copy(t - 1, prev).wait()
        a, b = front(slot)
        back(cb[lax.rem(t - 1, 2)], prev)
        cb[lax.rem(t, 2)] = gate(a, b)

        @pl.when(t - 1 + RING < steps)
        def _():
            start_weights(t - 1 + RING, prev)
        return 0

    def mlp2(i, _):
        t = 2 * i + 1
        s0, s1, s2 = lax.rem(t - 1, RING), lax.rem(t, RING), lax.rem(t + 1, RING)
        for c in front_copies(t, s1) + front_copies(t + 1, s2):
            c.wait()
        back_copy(t - 1, s0).wait()
        back_copy(t, s1).wait()
        a, b = front(s1)
        back(cb[0], s0)
        c1 = gate(a, b)
        a, b = front(s2)
        back(c1, s1)
        cb[0] = gate(a, b)
        for k, s in ((0, s0), (1, s1)):
            @pl.when(t - 1 + k + RING < steps)
            def _():
                start_weights(t - 1 + k + RING, s)
        return 0

    lax.fori_loop(0, (steps - 2) // 2, mlp2, 0)
    t = steps - 1
    for c in front_copies(t, t % RING):
        c.wait()
    back_copy(t - 1, (t - 1) % RING).wait()
    a, b = front(t % RING)
    back(cb[0], (t - 1) % RING)
    cb[1] = gate(a, b)
    last = (steps - 1) % RING
    back_copy(steps - 1, last).wait()
    c = cb[(steps - 1) % 2]
    for n in range(DN):
        sl = slice(n * W, (n + 1) * W)
        y = work[n] + jnp.dot(c, wd_v[last, :, sl], preferred_element_type=F32)
        ob[:, sl] = hb[:, sl] + y.astype(BF)
        pltpu.make_async_copy(ob.at[:, sl], out.at[:, sl], o_sem.at[n]).start()
    for n in range(DN):
        sl = slice(n * W, (n + 1) * W)
        pltpu.make_async_copy(ob.at[:, sl], out.at[:, sl], o_sem.at[n]).wait()


def solution(mesh):
    ANY = pl.BlockSpec(memory_space=pl.ANY)
    VM = pl.BlockSpec(memory_space=pltpu.VMEM)
    SM = pl.BlockSpec(memory_space=pltpu.SMEM)
    DMA = pltpu.SemaphoreType.DMA

    def body(hidden, seg_ids, norm_kv, w_key, w_value, norm_attn, w_query, w_out, norm_mlp, w_gate, w_up, w_down):
        wk = w_key.transpose(1, 2, 0).reshape(D, D)
        wv = w_value.transpose(1, 2, 0).reshape(D, D)
        wq = w_query[0].transpose(1, 2, 0).reshape(D, D)
        seg = seg_ids.reshape(1, T)
        row = jax.ShapeDtypeStruct((32, 1, T), F32)
        k_tiles = jax.ShapeDtypeStruct((16, G, H, W), BF)
        v_tiles = jax.ShapeDtypeStruct((16, G, W, H), BF)
        k4, v4, qt, seg_all, acc, m, l = pl.pallas_call(
            gather_kernel,
            out_shape=(k_tiles, v_tiles, jax.ShapeDtypeStruct((G, W, W), BF), jax.ShapeDtypeStruct((8, 1, T), jnp.int32),
                       jax.ShapeDtypeStruct((32, HD, T), F32), row, row),
            in_specs=[ANY, ANY, VM, VM, ANY, ANY, ANY],
            out_specs=(ANY,) * 7,
            scratch_shapes=[
                pltpu.VMEM((4, T, D), BF), *[pltpu.VMEM((D, D), BF)] * 4,
                pltpu.VMEM((T, D), BF), pltpu.VMEM((4, 2, G, H, W), BF), pltpu.VMEM((4, 2, G, W, H), BF),
                pltpu.VMEM((G, W, W), BF),
                DMA((3,)), DMA, *[DMA((4,))] * 6,
                *[DMA((7,))] * 2, DMA,
                DMA((4, 2)), *[DMA((4, GP, 2))] * 2, DMA((4, 2)), *[DMA((4, GP, 2))] * 2, DMA,
                pltpu.VMEM((2, G, H, W), BF), pltpu.VMEM((2, G, W, H), BF), pltpu.VMEM((8, 1, T), jnp.int32),
                pltpu.VMEM((T, T), F32), pltpu.VMEM((8, T, W), F32), pltpu.VMEM((8, 1, T), F32),
                pltpu.VMEM((32, 1, T), F32), pltpu.VMEM((32, 1, T), F32), pltpu.VMEM((32, HD, T), F32), DMA((5,)),
            ],
            compiler_params=pltpu.CompilerParams(collective_id=0, has_side_effects=True, vmem_limit_bytes=62 * 2 ** 20),
            cost_estimate=pl.CostEstimate(flops=20 * 10 ** 9, bytes_accessed=50 * 10 ** 6, transcendentals=0),
            name="gather_kv",
        )(hidden, seg, norm_kv, norm_attn, wk, wv, wq)

        return pl.pallas_call(
            layer_kernel,
            out_shape=jax.ShapeDtypeStruct((T, D), BF),
            in_specs=[SM] + [ANY] * 6 + [VM, ANY, VM, ANY, ANY, ANY, ANY],
            out_specs=ANY,
            scratch_shapes=[
                pltpu.VMEM((G, W, W), BF), pltpu.VMEM((KVS, 2, G, H, W), BF), pltpu.VMEM((KVS, 2, G, W, H), BF),
                pltpu.VMEM((T, T), F32), pltpu.VMEM((32, HD, T), F32), pltpu.VMEM((32, 1, T), F32), pltpu.VMEM((32, 1, T), F32), pltpu.VMEM((8, 1, T), F32),
                pltpu.VMEM((T, D), BF), pltpu.VMEM((T, D), BF), pltpu.VMEM((T, D), BF),
                pltpu.VMEM((D, D), BF), pltpu.VMEM((RING, D, FT), BF), pltpu.VMEM((RING, D, FT), BF), pltpu.VMEM((RING, FT, D), BF),
                pltpu.VMEM((2, T, FT), BF), pltpu.VMEM((8, T, W), F32),
                DMA, DMA((KVS, 2)), DMA, DMA((RING, 3)), DMA, DMA((DN,)), DMA((3,)),
            ],
            compiler_params=pltpu.CompilerParams(vmem_limit_bytes=63 * 2 ** 20),
            cost_estimate=pl.CostEstimate(flops=40 * 10 ** 9, bytes_accessed=130 * 10 ** 6, transcendentals=10 ** 7),
            name="layer",
        )(seg_all, qt, k4, v4, acc, m, l, seg_all, hidden, norm_mlp, w_out[0].reshape(D, D), w_gate[0], w_up[0], w_down[0])

    row_spec = P(('dp', 'sp'), None)
    in_specs = (row_spec, P(('dp', 'sp'))) + (P(),) * 10
    return jax.shard_map(body, mesh=mesh, in_specs=in_specs, out_specs=row_spec, check_vma=False)
```
